128 devices in a mesh: fsdp: 16 (over z, x), model: 8 (over y, core).
Axes of the slice: x: 4, y: 4, z: 4, core: 2. Of those that a mesh axis runs over, the one named last changes fastest.
Arguments:
- weight_query: bfloat16 [5120, 8192], P('fsdp', 'model'), may hold values from -0.125 to 0.125
- low_query: bfloat16 [5120, 32], P('fsdp'), may hold values from -0.078125 to 0.078125
- high_query: bfloat16 [32, 8192], P(None, 'model'), may hold values from -1 to 1
- weight_key: bfloat16 [5120, 1024], P('fsdp', 'model'), may hold values from -0.125 to 0.125
- low_key: bfloat16 [5120, 32], P('fsdp'), may hold values from -0.078125 to 0.078125
- high_key: bfloat16 [32, 1024], P(None, 'model'), may hold values from -1 to 1
- weight_value: bfloat16 [5120, 1024], P('fsdp', 'model'), may hold values from -0.125 to 0.125
- low_value: bfloat16 [5120, 32], P('fsdp'), may hold values from -0.078125 to 0.078125
- high_value: bfloat16 [32, 1024], P(None, 'model'), may hold values from -1 to 1
- norm_train: float32 [5120], P(('fsdp', 'model')), may hold values from 0.25 to 1.75
- norm_step: float32 [5120], P(('fsdp', 'model')), may hold values from -0.3 to 0.3
Outputs:
- final_query: bfloat16 [5120, 8192], P(None, 'model')
- final_key: bfloat16 [5120, 1024], P(None, 'model')
- final_value: bfloat16 [5120, 1024], P(None, 'model')
- column_query: float32 [8192], P('model')
- column_key: float32 [1024], P('model')
- column_value: float32 [1024], P('model')
- serve_norm: bfloat16 [5120], replicated
The draws below stay inside these ranges and needn't reach their ends.
All inputs are finite; a program needn't handle non-finite values. Where the reference program divides by a largest or mean magnitude, that divisor is 1e-20 or more.
Results may differ from the reference program's by a relative error of at most 0.001.
Values may be sent and summed in bfloat16 or wider, within the bound.
No kernel may reach another device: no remote copies, remote signals or barrier semaphores. Data moves between devices by JAX's collectives and lax.ppermute only.
A program may use at most 128 MiB of HBM per device.

```python
import jax
import jax.numpy as jnp

D_MODEL = 5120
Q_DIM = 8192
KV_DIM = 1024
RANK = 32


def strengthened(drawn, key, source, target, blocks, factor):
    owner, partner = [(jnp.arange(drawn.shape[dim]) // (drawn.shape[dim] // blocks)).reshape([-1 if axis == dim else 1 for axis in range(drawn.ndim)]) for dim in (source, target)]
    chosen = jax.random.permutation(key, blocks)[partner]
    strong = (owner == chosen) | (owner == (partner + blocks // 2) % blocks)
    return jnp.where(strong, factor * drawn, drawn)


def block_levels(key, dims, cuts, low, top_value):
    def one(axis_at, parts):
        draws = jax.random.uniform(jax.random.fold_in(jax.random.fold_in(key, 6), axis_at), (parts,), jnp.float32, low / len(cuts), top_value / len(cuts))
        return jnp.repeat(jnp.exp(draws), dims[axis_at] // parts).reshape((-1,) + (1,) * (len(dims) - axis_at - 1))

    loudness = one(*cuts[0])
    for cut in cuts[1:]:
        loudness = loudness * one(*cut)
    return loudness


def noise(own_key, dims, spread, reach, shards=(), dtype=jnp.bfloat16):
    array = spread * jax.random.normal(own_key, dims, jnp.float32)
    if shards:
        array = array * block_levels(own_key, dims, shards, -0.22, 0.18)
    return jnp.clip(array, -reach, reach).astype(dtype)


def bell_draw_with(own_key, dims, deviation, most, shards, heavy, kind=jnp.bfloat16):
    entries = deviation * jax.random.normal(own_key, dims, jnp.float32)
    if shards:
        entries = entries * block_levels(own_key, dims, shards, -0.22, 0.18)
    return jnp.clip(strengthened(entries, jax.random.fold_in(own_key, 3), *heavy), -most, most).astype(kind)


def setup_inputs(seed: int = 0) -> dict:
    seeds = jax.random.split(jax.random.key(seed), 12)
    weight_query = bell_draw_with(seeds[0], (D_MODEL, Q_DIM), D_MODEL ** -0.5, 0.125, ((0, 16), (1, 8)), (0, 1, 16, 2.0))
    low_query = noise(seeds[1], (D_MODEL, RANK), D_MODEL ** -0.5, 0.078125, ((0, 16),))
    high_query = noise(seeds[2], (RANK, Q_DIM), RANK ** -0.5, 1.0, ((1, 8),))
    weight_key = bell_draw_with(seeds[3], (D_MODEL, KV_DIM), D_MODEL ** -0.5, 0.125, ((0, 16), (1, 8)), (0, 1, 16, 2.0))
    low_key = noise(seeds[4], (D_MODEL, RANK), D_MODEL ** -0.5, 0.078125, ((0, 16),))
    high_key = noise(seeds[5], (RANK, KV_DIM), RANK ** -0.5, 1.0, ((1, 8),))
    weight_value = bell_draw_with(seeds[6], (D_MODEL, KV_DIM), D_MODEL ** -0.5, 0.125, ((0, 16), (1, 8)), (0, 1, 16, 2.0))
    low_value = noise(seeds[7], (D_MODEL, RANK), D_MODEL ** -0.5, 0.078125, ((0, 16),))
    high_value = noise(seeds[8], (RANK, KV_DIM), RANK ** -0.5, 1.0, ((1, 8),))
    norm_train = jnp.clip(1.0 + 0.15 * jax.random.normal(seeds[9], (D_MODEL,), jnp.float32), 0.25, 1.75)
    norm_step = jnp.clip(jax.random.uniform(seeds[10], (D_MODEL,), jnp.float32, -0.3, 0.3) * block_levels(seeds[10], (D_MODEL,), ((0, 128),), -0.4, 0.0), -0.3, 0.3)
    return dict(weight_query=weight_query, low_query=low_query, high_query=high_query, weight_key=weight_key, low_key=low_key, high_key=high_key, weight_value=weight_value, low_value=low_value, high_value=high_value, norm_train=norm_train, norm_step=norm_step)


mix_rate = 0.5


def reference(weight_query, low_query, high_query, weight_key, low_key, high_key, weight_value, low_value, high_value, norm_train, norm_step):
    result_query = weight_query.astype(jnp.float32) + mix_rate * jnp.dot(low_query, high_query, preferred_element_type=jnp.float32)
    result_key = weight_key.astype(jnp.float32) + mix_rate * jnp.dot(low_key, high_key, preferred_element_type=jnp.float32)
    result_value = weight_value.astype(jnp.float32) + mix_rate * jnp.dot(low_value, high_value, preferred_element_type=jnp.float32)
    column_query = jnp.max(jnp.abs(result_query), axis=0)
    final_query = (result_query / column_query).astype(jnp.bfloat16)
    column_key = jnp.max(jnp.abs(result_key), axis=0)
    final_key = (result_key / column_key).astype(jnp.bfloat16)
    column_value = jnp.max(jnp.abs(result_value), axis=0)
    final_value = (result_value / column_value).astype(jnp.bfloat16)
    serve_norm = (norm_train + norm_step).astype(jnp.bfloat16)
    return final_query, final_key, final_value, column_query, column_key, column_value, serve_norm
```

```python
import jax
import jax.numpy as jnp
from jax import lax
from jax.experimental import pallas as pl
from jax.experimental.pallas import tpu as pltpu
from jax.sharding import PartitionSpec as P

mix_rate = 0.5
SIDE = 4


def x_ring(step):
    return [(z * SIDE + x, z * SIDE + (x + step) % SIDE) for z in range(SIDE) for x in range(SIDE)]


def z_ring(step):
    return [(z * SIDE + x, (z + step) % SIDE * SIDE + x) for z in range(SIDE) for x in range(SIDE)]


RING = {"x": x_ring, "z": z_ring}


def wrapped(offset):
    return (offset + 1) % SIDE - 1


class Units:
    def __init__(self, array, places):
        self.array, self.places = array, places

    def moved(self, axis, step):
        array = lax.ppermute(self.array, "fsdp", RING[axis](step))
        if axis == "x":
            places = [(wrapped(ox - step), oz, h, k) for ox, oz, h, k in self.places]
        else:
            places = [(ox, wrapped(oz - step), h, k) for ox, oz, h, k in self.places]
        return Units(array, places)

    def take(self, first, count, unit):
        return Units(self.array[first * unit : (first + count) * unit], self.places[first : first + count])


def joined(parts):
    return Units(jnp.concatenate([p.array for p in parts], axis=0), sum((p.places for p in parts), []))


def spread(block):
    unit = block.shape[0] // 4
    half = {h: Units(block[2 * h * unit : 2 * (h + 1) * unit], [(0, 0, h, 0), (0, 0, h, 1)]) for h in (0, 1)}
    ways = [("x", 1), ("x", -1), ("z", 1), ("z", -1)]
    lead = {"x": 0, "z": 1}
    other = {"x": "z", "z": "x"}
    quarter = {1: 0, -1: 1}
    kept = [half[0], half[1]]
    a = {(ax, s): half[lead[ax]].moved(ax, s) for ax, s in ways}
    b = {(ax, s): half[1 - lead[ax]].moved(ax, s) for ax, s in ways}
    kept += [*a.values(), *b.values()]
    c = {}
    for ax, s in ways:
        o = other[ax]
        c[ax, s] = joined([a[ax, s].take(quarter[s], 1, unit), a[o, 1], a[o, -1]]).moved(ax, s)
    d = {(ax, s): b[ax, s].take(quarter[s], 1, unit).moved(ax, s) for ax, s in ways}
    kept += [*c.values(), *d.values()]
    e, f = {}, {}
    for ax, s in ways:
        o = other[ax]
        e[ax, s] = joined([c[o, 1].take(0, 1, unit), c[o, -1].take(0, 1, unit)]).moved(ax, s)
        q = quarter[s]
        f[ax, s] = joined([c[ax, s].take(1 + q, 1, unit), c[ax, s].take(3 + q, 1, unit)]).moved(ax, s)
    kept += [*e.values(), *f.values()]
    g = {(ax, s): e[ax, s].take(quarter[s], 1, unit).moved(ax, s) for ax, s in ways}
    kept += [*g.values()]
    return kept, unit


def placed(kept, unit, widths):
    total = 4 * SIDE * SIDE * unit
    count = len(kept)
    assert sorted(p for u in kept for p in u.places) == sorted(
        (ox, oz, h, k) for ox in (-1, 0, 1, 2) for oz in (-1, 0, 1, 2) for h in (0, 1) for k in (0, 1)
    )

    def body(*refs):
        ins, outs, sems = refs[:count], refs[count : count + len(widths)], refs[-1]
        me = lax.axis_index("fsdp")
        z, x = me // SIDE, me % SIDE
        for ref, units in zip(ins, kept):
            for j, (ox, oz, h, k) in enumerate(units.places):
                source = (z + oz + SIDE) % SIDE * SIDE + (x + ox + SIDE) % SIDE
                row = pl.multiple_of((source * 4 + h * 2 + k) * unit, unit)
                at = 0
                for n, width in enumerate(widths):
                    pltpu.make_async_copy(
                        ref.at[pl.ds(j * unit, unit), pl.ds(at, width)], outs[n].at[pl.ds(row, unit), :], sems.at[n]
                    ).start()
                    at += width
        for n in range(len(widths)):
            pltpu.make_async_copy(outs[n], outs[n], sems.at[n]).wait()

    return pl.pallas_call(
        body,
        out_shape=[jax.ShapeDtypeStruct((total, width), kept[0].array.dtype) for width in widths],
        in_specs=[pl.BlockSpec(memory_space=pl.ANY)] * count,
        out_specs=[pl.BlockSpec(memory_space=pl.ANY)] * len(widths),
        scratch_shapes=[pltpu.SemaphoreType.DMA((len(widths),))],
        name="placed",
    )(*[u.array for u in kept])


def row_and_column_max(values):
    for ring in (x_ring, z_ring):
        values = jnp.maximum(
            jnp.maximum(values, lax.ppermute(values, "fsdp", ring(2))),
            jnp.maximum(lax.ppermute(values, "fsdp", ring(1)), lax.ppermute(values, "fsdp", ring(-1))),
        )
    return values


def per_device(
    weight_query,
    low_query,
    high_query,
    weight_key,
    low_key,
    high_key,
    weight_value,
    low_value,
    high_value,
    norm_train,
    norm_step,
):
    me = lax.axis_index("fsdp")
    lane = lax.axis_index("model")
    groups, lanes = lax.axis_size("fsdp"), lax.axis_size("model")
    results = [
        w.astype(jnp.float32) + mix_rate * jnp.dot(low, high, preferred_element_type=jnp.float32)
        for w, low, high in (
            (weight_query, low_query, high_query),
            (weight_key, low_key, high_key),
            (weight_value, low_value, high_value),
        )
    ]
    widths = [r.shape[1] for r in results]
    wide = sum(widths)
    norm = (norm_train + norm_step).astype(jnp.bfloat16).astype(jnp.float32)
    slots = jnp.where(jnp.arange(groups)[:, None] == me, norm[None, :], -jnp.inf).reshape(-1)
    shared = row_and_column_max(jnp.concatenate([*[jnp.max(jnp.abs(r), axis=0) for r in results], slots]))
    columns, at = [], 0
    for width in widths:
        columns.append(shared[at : at + width])
        at += width
    block = jnp.concatenate([(r / c).astype(jnp.bfloat16) for r, c in zip(results, columns)], axis=1)
    kept, unit = spread(block)
    finals = placed(kept, unit, widths)
    mine = shared[wide:].astype(jnp.bfloat16).reshape(groups, 1, -1)
    gains = jnp.where((jnp.arange(lanes) == lane)[None, :, None], mine, -jnp.inf).reshape(-1)
    for bit in (1, 2, 4):
        gains = jnp.maximum(gains, lax.ppermute(gains, "model", [(i, i ^ bit) for i in range(lanes)]))
    return (*finals, *columns, gains)


def solution(mesh):
    return jax.shard_map(
        per_device,
        mesh=mesh,
        in_specs=(
            P("fsdp", "model"),
            P("fsdp", None),
            P(None, "model"),
            P("fsdp", "model"),
            P("fsdp", None),
            P(None, "model"),
            P("fsdp", "model"),
            P("fsdp", None),
            P(None, "model"),
            P(("fsdp", "model")),
            P(("fsdp", "model")),
        ),
        out_specs=(
            P(None, "model"),
            P(None, "model"),
            P(None, "model"),
            P("model"),
            P("model"),
            P("model"),
            P(),
        ),
        check_vma=False,
    )
```

```python
import jax
import jax.numpy as jnp
from jax import lax
from jax.experimental import pallas as pl
from jax.experimental.pallas import tpu as pltpu
from jax.sharding import PartitionSpec as P


mix_rate = 0.5
SIDE = 4
LANES = 128


def x_ring(step):
    return [(z * SIDE + x, z * SIDE + (x + step) % SIDE) for z in range(SIDE) for x in range(SIDE)]


def z_ring(step):
    return [(z * SIDE + x, (z + step) % SIDE * SIDE + x) for z in range(SIDE) for x in range(SIDE)]


RING = {"x": x_ring, "z": z_ring}


def wrapped(offset):
    return (offset + 1) % SIDE - 1


WAYS = [("x", 1), ("x", -1), ("z", 1), ("z", -1)]
LEAD = {"x": 0, "z": 1}
OTHER = {"x": "z", "z": "x"}
QUARTER = {1: 0, -1: 1}


def sent(array, axis, step):
    return lax.ppermute(array, "fsdp", RING[axis](step))


def all_ways(message):
    return {(ax, s): sent(message(ax, s), ax, s) for ax, s in WAYS}


def shifted(place, axis, step):
    ox, oz, h, k = place
    return (wrapped(ox - step), oz, h, k) if axis == "x" else (ox, wrapped(oz - step), h, k)


def pair(half, axis=None, step=0):
    places = [(0, 0, half, 0), (0, 0, half, 1)]
    return [shifted(p, axis, step) for p in places] if axis else places


def a_places(ax, s):
    return pair(LEAD[ax], ax, s)


def b_places(ax, s):
    return pair(1 - LEAD[ax], ax, s)


def c_message_places(ax, s):
    o = OTHER[ax]
    return [a_places(ax, s)[QUARTER[s]], *a_places(o, 1), *a_places(o, -1)]


def c_places(ax, s):
    return [shifted(p, ax, s) for p in c_message_places(ax, s)]


def d_places(ax, s):
    return [shifted(b_places(ax, s)[QUARTER[s]], ax, s)]


def e_message_places(ax):
    o = OTHER[ax]
    return [c_places(o, 1)[0], c_places(o, -1)[0]]


def e_places(ax, s):
    return [shifted(p, ax, s) for p in e_message_places(ax)]


def f_places(ax, s):
    held, q = c_places(ax, s), QUARTER[s]
    return [shifted(held[1 + q], ax, s), shifted(held[3 + q], ax, s)]


def g_places(ax, s):
    return [shifted(e_places(ax, s)[QUARTER[s]], ax, s)]


HBM = pl.BlockSpec(memory_space=pl.ANY)
VMEM = pl.BlockSpec(memory_space=pltpu.VMEM)


def in_vmem(array):
    return pltpu.with_memory_space_constraint(array, pltpu.VMEM)


def row_of(place, unit):
    me = lax.axis_index("fsdp")
    z, x = me // SIDE, me % SIDE
    ox, oz, h, k = place
    source = (z + oz + SIDE) % SIDE * SIDE + (x + ox + SIDE) % SIDE
    return pl.multiple_of((source * 4 + h * 2 + k) * unit, unit)


def runs(places):
    out, at = [], 0
    while at < len(places):
        ox, oz, h, k = places[at]
        size = 2 if k == 0 and at + 1 < len(places) and places[at + 1] == (ox, oz, h, 1) else 1
        out.append((at, size, places[at]))
        at += size
    return out


def column_copies(ref, first, rows, results, row, widths, sems):
    at = 0
    for n, width in enumerate(widths):
        pltpu.make_async_copy(
            ref.at[pl.ds(first, rows), pl.ds(at, width)], results[n].at[pl.ds(row, rows), :], sems.at[n]
        ).start()
        at += width


def wait_for(rows, results, sems):
    for n, result in enumerate(results):
        part = result.at[pl.ds(0, rows), :]
        pltpu.make_async_copy(part, part, sems.at[n]).wait()


def merged_into(raw, first, rows, mixed_ref, inverse_ref, targets, wide):
    low = raw[pl.ds(first, rows), pl.ds(wide, LANES)]
    tile = 2 * LANES
    for t in range(0, wide, tile):
        update = jnp.dot(low, mixed_ref[:, t : t + tile], preferred_element_type=jnp.float32)
        value = (raw[pl.ds(first, rows), t : t + tile].astype(jnp.float32) + update) * inverse_ref[:, t : t + tile]
        value = value.astype(jnp.bfloat16)
        for ref, at, skip, size in targets:
            ref[pl.ds(at, size), t : t + tile] = value[skip : skip + size]


def first_hop(a, unit, mixed, inverse, widths):
    wide, total = sum(widths), 4 * SIDE * SIDE * unit
    order = {way: n for n, way in enumerate(WAYS)}

    def body(*refs):
        mixed_ref, inverse_ref, raws = refs[0], refs[1], refs[2:6]
        messages, results, sems = refs[6:10], refs[10 : 10 + len(widths)], refs[-1]
        for ax, s in WAYS:
            o, q = OTHER[ax], QUARTER[s]
            at = (1 + 2 * q) * unit
            targets = [
                (messages[order[ax, s]], 0, q * unit, unit),
                (messages[order[o, 1]], at, 0, 2 * unit),
                (messages[order[o, -1]], at, 0, 2 * unit),
            ]
            merged_into(raws[order[ax, s]], 0, 2 * unit, mixed_ref, inverse_ref, targets, wide)
            column_copies(
                messages[order[o, 1]], at, 2 * unit, results, row_of(a_places(ax, s)[0], unit), widths, sems
            )
        wait_for(8 * unit, results, sems)

    out = pl.pallas_call(
        body,
        out_shape=[jax.ShapeDtypeStruct((5 * unit, wide), jnp.bfloat16)] * 4
        + [jax.ShapeDtypeStruct((total, width), jnp.bfloat16) for width in widths],
        in_specs=[VMEM] * 6,
        out_specs=[VMEM] * 4 + [HBM] * len(widths),
        scratch_shapes=[pltpu.SemaphoreType.DMA((len(widths),))],
        compiler_params=pltpu.CompilerParams(vmem_limit_bytes=20 * 2**20),
        name="first_hop",
    )(mixed, inverse, *[in_vmem(a[way]) for way in WAYS])
    return {way: out[n] for n, way in enumerate(WAYS)}, out[4:]


def second_hop(b, own, unit, mixed, inverse, finals, widths):
    wide = sum(widths)

    def body(*refs):
        mixed_ref, inverse_ref, raws, own_ref = refs[0], refs[1], refs[2:6], refs[6]
        messages = refs[7 + len(widths) : 11 + len(widths)]
        results, stage, sems = refs[11 + len(widths) : -2], refs[-2], refs[-1]
        for n, (ax, s) in enumerate(WAYS):
            q = QUARTER[s]
            at = 2 * n * unit
            targets = [(messages[n], 0, q * unit, unit), (stage, at, 0, 2 * unit)]
            merged_into(raws[n], 0, 2 * unit, mixed_ref, inverse_ref, targets, wide)
            column_copies(stage, at, 2 * unit, results, row_of(b_places(ax, s)[0], unit), widths, sems)
        for h in (0, 1):
            at = (8 + 2 * h) * unit
            merged_into(own_ref, 2 * h * unit, 2 * unit, mixed_ref, inverse_ref, [(stage, at, 0, 2 * unit)], wide)
            column_copies(stage, at, 2 * unit, results, row_of((0, 0, h, 0), unit), widths, sems)
        wait_for(12 * unit, results, sems)

    out = pl.pallas_call(
        body,
        out_shape=[jax.ShapeDtypeStruct((unit, wide), jnp.bfloat16)] * 4
        + [jax.ShapeDtypeStruct(f.shape, f.dtype) for f in finals],
        in_specs=[VMEM] * 7 + [HBM] * len(widths),
        out_specs=[VMEM] * 4 + [HBM] * len(widths),
        scratch_shapes=[pltpu.VMEM((12 * unit, wide), jnp.bfloat16), pltpu.SemaphoreType.DMA((len(widths),))],
        input_output_aliases={7 + n: 4 + n for n in range(len(widths))},
        compiler_params=pltpu.CompilerParams(vmem_limit_bytes=20 * 2**20),
        name="second_hop",
    )(mixed, inverse, *[in_vmem(b[way]) for way in WAYS], in_vmem(own), *finals)
    return {way: out[n] for n, way in enumerate(WAYS)}, out[4:]


def placed(groups, unit, finals, widths):
    arrays = [array for array, _ in groups]
    count = len(arrays)

    def body(*refs):
        results, sems = refs[-1 - len(widths) : -1], refs[-1]
        rows = 0
        for ref, (_, places) in zip(refs[:count], groups):
            for at, size, place in runs(places):
                column_copies(ref, at * unit, size * unit, results, row_of(place, unit), widths, sems)
            rows += len(places) * unit
        wait_for(rows, results, sems)

    return pl.pallas_call(
        body,
        out_shape=[jax.ShapeDtypeStruct(f.shape, f.dtype) for f in finals],
        in_specs=[VMEM] * count + [HBM] * len(widths),
        out_specs=[HBM] * len(widths),
        scratch_shapes=[pltpu.SemaphoreType.DMA((len(widths),))],
        input_output_aliases={count + n: n for n in range(len(widths))},
        compiler_params=pltpu.CompilerParams(vmem_limit_bytes=8 * 2**20),
    )(*[in_vmem(array) for array in arrays], *finals)


def round_of_max(values, ring):
    others = []
    for step in (2, 1, -1):
        others.append(lax.ppermute(values, "fsdp", ring(step)))
    return jnp.maximum(jnp.maximum(values, others[0]), jnp.maximum(others[1], others[2]))


def per_device(
    weight_query,
    low_query,
    high_query,
    weight_key,
    low_key,
    high_key,
    weight_value,
    low_value,
    high_value,
    norm_train,
    norm_step,
):
    me = lax.axis_index("fsdp")
    lane = lax.axis_index("model")
    groups, lanes = lax.axis_size("fsdp"), lax.axis_size("model")
    weights = (weight_query, weight_key, weight_value)
    lows = (low_query, low_key, low_value)
    highs = (high_query, high_key, high_value)
    widths = [w.shape[1] for w in weights]
    wide, ranks = sum(widths), [low.shape[1] for low in lows]
    rows = weight_query.shape[0]
    unit = rows // 4
    rest = LANES - sum(ranks)
    block = jnp.concatenate([*weights, *lows, jnp.zeros((rows, rest), jnp.bfloat16)], axis=1)
    halves = [block[: 2 * unit], block[2 * unit :]]
    a = all_ways(lambda ax, s: halves[LEAD[ax]])
    b = all_ways(lambda ax, s: halves[1 - LEAD[ax]])

    largest = [
        jnp.max(
            jnp.abs(w.astype(jnp.float32) + mix_rate * jnp.dot(low, high, preferred_element_type=jnp.float32)),
            axis=0,
        )
        for w, low, high in zip(weights, lows, highs)
    ]
    norm = (norm_train + norm_step).astype(jnp.bfloat16).astype(jnp.float32)
    slots = jnp.where(jnp.arange(groups)[:, None] == me, norm[None, :], -jnp.inf).reshape(-1)
    shared = round_of_max(jnp.concatenate([*largest, slots]), z_ring)
    shared = round_of_max(shared, x_ring)
    columns, at = [], 0
    for width in widths:
        columns.append(shared[at : at + width])
        at += width
    inverse = (1.0 / shared[:wide]).reshape(1, wide)
    mixed, at = [], 0
    for high, width in zip(highs, widths):
        mixed.append(jnp.pad(mix_rate * high, ((0, 0), (at, wide - at - width))))
        at += width
    mixed = jnp.concatenate([*mixed, jnp.zeros((rest, wide), jnp.bfloat16)], axis=0)

    messages, finals = first_hop(a, unit, mixed, inverse, widths)
    c = all_ways(lambda ax, s: messages[ax, s])
    messages, finals = second_hop(b, block, unit, mixed, inverse, finals, widths)
    d = all_ways(lambda ax, s: messages[ax, s])

    mine = shared[wide:].astype(jnp.bfloat16).reshape(groups, 1, -1)
    gains = jnp.where((jnp.arange(lanes) == lane)[None, :, None], mine, -jnp.inf).reshape(-1)
    for n in range(3):
        gains = jnp.maximum(gains, lax.ppermute(gains, "model", [(i, i ^ 2**n) for i in range(lanes)]))

    along = {ax: jnp.concatenate([c[OTHER[ax], 1][:unit], c[OTHER[ax], -1][:unit]]) for ax in "xz"}
    e = all_ways(lambda ax, s: along[ax])

    def forwarded(ax, s):
        held, q = c[ax, s], QUARTER[s]
        return jnp.concatenate([held[(1 + q) * unit : (2 + q) * unit], held[(3 + q) * unit : (4 + q) * unit]])

    f = all_ways(forwarded)
    g = all_ways(lambda ax, s: e[ax, s][QUARTER[s] * unit : (QUARTER[s] + 1) * unit])
    finals = placed([(d[w], d_places(*w)) for w in WAYS], unit, finals, widths)
    finals = placed([(c[w], c_places(*w)) for w in WAYS], unit, finals, widths)
    finals = placed([(e[w], e_places(*w)) for w in WAYS] + [(f[w], f_places(*w)) for w in WAYS], unit, finals, widths)
    finals = placed([(g[w], g_places(*w)) for w in WAYS], unit, finals, widths)
    return (*finals, *columns, gains)


def solution(mesh):
    return jax.shard_map(
        per_device,
        mesh=mesh,
        in_specs=(
            P("fsdp", "model"),
            P("fsdp", None),
            P(None, "model"),
            P("fsdp", "model"),
            P("fsdp", None),
            P(None, "model"),
            P("fsdp", "model"),
            P("fsdp", None),
            P(None, "model"),
            P(("fsdp", "model")),
            P(("fsdp", "model")),
        ),
        out_specs=(
            P(None, "model"),
            P(None, "model"),
            P(None, "model"),
            P("model"),
            P("model"),
            P("model"),
            P(),
        ),
        check_vma=False,
    )
```

```python
import jax
import jax.numpy as jnp
from jax import lax
from jax.experimental import pallas as pl
from jax.experimental.pallas import tpu as pltpu
from jax.sharding import PartitionSpec as P


mix_rate = 0.5
SIDE = 4
LANES = 128


def x_ring(step):
    return [(z * SIDE + x, z * SIDE + (x + step) % SIDE) for z in range(SIDE) for x in range(SIDE)]


def z_ring(step):
    return [(z * SIDE + x, (z + step) % SIDE * SIDE + x) for z in range(SIDE) for x in range(SIDE)]


RING = {"x": x_ring, "z": z_ring}


def wrapped(offset):
    return (offset + 1) % SIDE - 1


WAYS = [("x", 1), ("x", -1), ("z", 1), ("z", -1)]
LEAD = {"x": 0, "z": 1}
OTHER = {"x": "z", "z": "x"}
QUARTER = {1: 0, -1: 1}


def sent(array, axis, step):
    return lax.ppermute(array, "fsdp", RING[axis](step))


def all_ways(message):
    return {(ax, s): sent(message(ax, s), ax, s) for ax, s in WAYS}


def shifted(place, axis, step):
    ox, oz, h, k = place
    return (wrapped(ox - step), oz, h, k) if axis == "x" else (ox, wrapped(oz - step), h, k)


def pair(half, axis=None, step=0):
    places = [(0, 0, half, 0), (0, 0, half, 1)]
    return [shifted(p, axis, step) for p in places] if axis else places


def a_places(ax, s):
    return pair(LEAD[ax], ax, s)


def b_places(ax, s):
    return pair(1 - LEAD[ax], ax, s)


def c_message_places(ax, s):
    o = OTHER[ax]
    return [a_places(ax, s)[QUARTER[s]], *a_places(o, 1), *a_places(o, -1)]


def c_places(ax, s):
    return [shifted(p, ax, s) for p in c_message_places(ax, s)]


def d_places(ax, s):
    return [shifted(b_places(ax, s)[QUARTER[s]], ax, s)]


def e_message_places(ax):
    o = OTHER[ax]
    return [c_places(o, 1)[0], c_places(o, -1)[0]]


def e_places(ax, s):
    return [shifted(p, ax, s) for p in e_message_places(ax)]


def f_places(ax, s):
    held, q = c_places(ax, s), QUARTER[s]
    return [shifted(held[1 + q], ax, s), shifted(held[3 + q], ax, s)]


def g_places(ax, s):
    return [shifted(e_places(ax, s)[QUARTER[s]], ax, s)]


HBM = pl.BlockSpec(memory_space=pl.ANY)
VMEM = pl.BlockSpec(memory_space=pltpu.VMEM)


def in_vmem(array):
    return pltpu.with_memory_space_constraint(array, pltpu.VMEM)


def row_of(place, unit):
    me = lax.axis_index("fsdp")
    z, x = me // SIDE, me % SIDE
    ox, oz, h, k = place
    source = (z + oz + SIDE) % SIDE * SIDE + (x + ox + SIDE) % SIDE
    return pl.multiple_of((source * 4 + h * 2 + k) * unit, unit)


def runs(places):
    out, at = [], 0
    while at < len(places):
        ox, oz, h, k = places[at]
        size = 2 if k == 0 and at + 1 < len(places) and places[at + 1] == (ox, oz, h, 1) else 1
        out.append((at, size, places[at]))
        at += size
    return out


def column_copies(ref, first, rows, results, row, widths, sems):
    at = 0
    for n, width in enumerate(widths):
        pltpu.make_async_copy(
            ref.at[pl.ds(first, rows), pl.ds(at, width)], results[n].at[pl.ds(row, rows), :], sems.at[n]
        ).start()
        at += width


def wait_for(rows, results, sems):
    for n, result in enumerate(results):
        part = result.at[pl.ds(0, rows), :]
        pltpu.make_async_copy(part, part, sems.at[n]).wait()


def merged_into(raw, first, rows, mixed_ref, inverse_ref, targets, wide):
    low = raw[pl.ds(first, rows), pl.ds(wide, LANES)]
    tile = 2 * LANES
    for t in range(0, wide, tile):
        update = jnp.dot(low, mixed_ref[:, t : t + tile], preferred_element_type=jnp.float32)
        value = (raw[pl.ds(first, rows), t : t + tile].astype(jnp.float32) + update) * inverse_ref[:, t : t + tile]
        value = value.astype(jnp.bfloat16)
        for ref, at, skip, size in targets:
            ref[pl.ds(at, size), t : t + tile] = value[skip : skip + size]


def first_hop(a, unit, mixed, inverse, widths):
    wide, total = sum(widths), 4 * SIDE * SIDE * unit
    order = {way: n for n, way in enumerate(WAYS)}

    def body(*refs):
        mixed_ref, inverse_ref, raws = refs[0], refs[1], refs[2:6]
        messages, results, sems = refs[6:10], refs[10 : 10 + len(widths)], refs[-1]
        for ax, s in WAYS:
            o, q = OTHER[ax], QUARTER[s]
            at = (1 + 2 * q) * unit
            targets = [
                (messages[order[ax, s]], 0, q * unit, unit),
                (messages[order[o, 1]], at, 0, 2 * unit),
                (messages[order[o, -1]], at, 0, 2 * unit),
            ]
            merged_into(raws[order[ax, s]], 0, 2 * unit, mixed_ref, inverse_ref, targets, wide)
            column_copies(
                messages[order[o, 1]], at, 2 * unit, results, row_of(a_places(ax, s)[0], unit), widths, sems
            )
        wait_for(8 * unit, results, sems)

    out = pl.pallas_call(
        body,
        out_shape=[jax.ShapeDtypeStruct((5 * unit, wide), jnp.bfloat16)] * 4
        + [jax.ShapeDtypeStruct((total, width), jnp.bfloat16) for width in widths],
        in_specs=[VMEM] * 6,
        out_specs=[VMEM] * 4 + [HBM] * len(widths),
        scratch_shapes=[pltpu.SemaphoreType.DMA((len(widths),))],
        compiler_params=pltpu.CompilerParams(vmem_limit_bytes=8 * 2**20),
        name="first_hop",
    )(mixed, inverse, *[in_vmem(a[way]) for way in WAYS])
    return {way: out[n] for n, way in enumerate(WAYS)}, out[4:]


def second_hop(b, own, unit, mixed, inverse, finals, widths):
    wide = sum(widths)

    def body(*refs):
        mixed_ref, inverse_ref, raws, own_refs = refs[0], refs[1], refs[2:6], refs[6:8]
        messages = refs[8 + len(widths) : 12 + len(widths)]
        results, stage, sems = refs[12 + len(widths) : -2], refs[-2], refs[-1]
        for n, (ax, s) in enumerate(WAYS):
            q = QUARTER[s]
            at = 2 * n * unit
            targets = [(messages[n], 0, q * unit, unit), (stage, at, 0, 2 * unit)]
            merged_into(raws[n], 0, 2 * unit, mixed_ref, inverse_ref, targets, wide)
            column_copies(stage, at, 2 * unit, results, row_of(b_places(ax, s)[0], unit), widths, sems)
        for h in (0, 1):
            at = (8 + 2 * h) * unit
            merged_into(own_refs[h], 0, 2 * unit, mixed_ref, inverse_ref, [(stage, at, 0, 2 * unit)], wide)
            column_copies(stage, at, 2 * unit, results, row_of((0, 0, h, 0), unit), widths, sems)
        wait_for(12 * unit, results, sems)

    out = pl.pallas_call(
        body,
        out_shape=[jax.ShapeDtypeStruct((unit, wide), jnp.bfloat16)] * 4
        + [jax.ShapeDtypeStruct(f.shape, f.dtype) for f in finals],
        in_specs=[VMEM] * 8 + [HBM] * len(widths),
        out_specs=[VMEM] * 4 + [HBM] * len(widths),
        scratch_shapes=[pltpu.VMEM((12 * unit, wide), jnp.bfloat16), pltpu.SemaphoreType.DMA((len(widths),))],
        input_output_aliases={8 + n: 4 + n for n in range(len(widths))},
        compiler_params=pltpu.CompilerParams(vmem_limit_bytes=8 * 2**20),
        name="second_hop",
    )(mixed, inverse, *[in_vmem(b[way]) for way in WAYS], *[in_vmem(half) for half in own], *finals)
    return {way: out[n] for n, way in enumerate(WAYS)}, out[4:]


def placed(groups, unit, finals, widths):
    arrays = [array for array, _ in groups]
    count = len(arrays)

    def body(*refs):
        results, sems = refs[-1 - len(widths) : -1], refs[-1]
        rows = 0
        for ref, (_, places) in zip(refs[:count], groups):
            for at, size, place in runs(places):
                column_copies(ref, at * unit, size * unit, results, row_of(place, unit), widths, sems)
            rows += len(places) * unit
        wait_for(rows, results, sems)

    return pl.pallas_call(
        body,
        out_shape=[jax.ShapeDtypeStruct(f.shape, f.dtype) for f in finals],
        in_specs=[VMEM] * count + [HBM] * len(widths),
        out_specs=[HBM] * len(widths),
        scratch_shapes=[pltpu.SemaphoreType.DMA((len(widths),))],
        input_output_aliases={count + n: n for n in range(len(widths))},
        compiler_params=pltpu.CompilerParams(vmem_limit_bytes=8 * 2**20),
    )(*[in_vmem(array) for array in arrays], *finals)


def packed(weights, lows, widths):
    rows, wide = weights[0].shape[0], sum(widths)
    half, rank, count = rows // 2, lows[0].shape[1], len(weights)

    def body(*refs):
        sources, turned, outs = refs[:count], refs[count : 2 * count], refs[2 * count : 2 * count + 2]
        stage, sems = refs[-2], refs[-1]
        low_copies = [
            pltpu.make_async_copy(turned[n], stage.at[n], sems.at[n])
            for n in range(count)
        ]
        for copy in low_copies:
            copy.start()
        copies, at = [], 0
        for n, width in enumerate(widths):
            for h in (0, 1):
                copies.append(
                    pltpu.make_async_copy(
                        sources[n].at[pl.ds(h * half, half), :],
                        outs[h].at[:, pl.ds(at, width)],
                        sems.at[count + 2 * n + h],
                    )
                )
                copies[-1].start()
            at += width
        for copy in low_copies:
            copy.wait()
        low = jnp.concatenate(
            [stage[n].astype(jnp.float32) for n in range(count)]
            + [jnp.zeros((LANES - count * rank, rows), jnp.float32)]
        )
        straight = low.T.astype(stage.dtype)
        for h in (0, 1):
            outs[h][:, wide:] = straight[h * half : (h + 1) * half]
        for copy in copies:
            copy.wait()

    return pl.pallas_call(
        body,
        out_shape=[jax.ShapeDtypeStruct((half, wide + LANES), jnp.bfloat16)] * 2,
        in_specs=[pl.BlockSpec(memory_space=pltpu.MemorySpace.HBM)] * (2 * count),
        out_specs=[VMEM] * 2,
        scratch_shapes=[pltpu.VMEM((count, rank, rows), jnp.bfloat16), pltpu.SemaphoreType.DMA((3 * count,))],
        compiler_params=pltpu.CompilerParams(vmem_limit_bytes=4 * 2**20),
        name="packed",
    )(*[pltpu.with_memory_space_constraint(a, pltpu.MemorySpace.HBM) for a in (*weights, *[low.T for low in lows])])


def round_of_max(values, ring):
    others = []
    for step in (2, 1, -1):
        others.append(lax.ppermute(values, "fsdp", ring(step)))
    return jnp.maximum(jnp.maximum(values, others[0]), jnp.maximum(others[1], others[2]))


def per_device(
    weight_query,
    low_query,
    high_query,
    weight_key,
    low_key,
    high_key,
    weight_value,
    low_value,
    high_value,
    norm_train,
    norm_step,
):
    me = lax.axis_index("fsdp")
    lane = lax.axis_index("model")
    groups, lanes = lax.axis_size("fsdp"), lax.axis_size("model")
    weights = (weight_query, weight_key, weight_value)
    lows = (low_query, low_key, low_value)
    highs = (high_query, high_key, high_value)
    widths = [w.shape[1] for w in weights]
    wide, ranks = sum(widths), [low.shape[1] for low in lows]
    rows = weight_query.shape[0]
    unit = rows // 4
    rest = LANES - sum(ranks)
    norm = (norm_train + norm_step).astype(jnp.bfloat16).astype(jnp.float32)
    slots = lax.dynamic_update_slice(
        jnp.full((groups * lanes * norm.shape[0],), -jnp.inf), norm, ((me * lanes + lane) * norm.shape[0],)
    )
    halves = packed(weights, lows, widths)
    a = all_ways(lambda ax, s: halves[LEAD[ax]])
    b = all_ways(lambda ax, s: halves[1 - LEAD[ax]])

    largest = [
        jnp.max(
            jnp.abs(w.astype(jnp.float32) + mix_rate * jnp.dot(low, high, preferred_element_type=jnp.float32)),
            axis=0,
        )
        for w, low, high in zip(weights, lows, highs)
    ]
    shared = round_of_max(jnp.concatenate([*largest, slots]), z_ring)
    shared = round_of_max(shared, x_ring)
    columns, at = [], 0
    for width in widths:
        columns.append(shared[at : at + width])
        at += width
    inverse = (1.0 / shared[:wide]).reshape(1, wide)
    mixed, at = [], 0
    for high, width in zip(highs, widths):
        mixed.append(jnp.pad(mix_rate * high, ((0, 0), (at, wide - at - width))))
        at += width
    mixed = jnp.concatenate([*mixed, jnp.zeros((rest, wide), jnp.bfloat16)], axis=0)

    messages, finals = first_hop(a, unit, mixed, inverse, widths)
    c = all_ways(lambda ax, s: messages[ax, s])
    messages, finals = second_hop(b, halves, unit, mixed, inverse, finals, widths)
    d = all_ways(lambda ax, s: messages[ax, s])

    gains = shared[wide:]
    for n in range(3):
        other = lax.ppermute(gains, "model", [(i, i ^ 2**n) for i in range(lanes)])
        gains = jnp.maximum(gains, other)
        if n == 2:
            gains = gains.astype(jnp.bfloat16)

    along = {ax: jnp.concatenate([c[OTHER[ax], 1][:unit], c[OTHER[ax], -1][:unit]]) for ax in "xz"}
    e = all_ways(lambda ax, s: along[ax])

    def forwarded(ax, s):
        held, q = c[ax, s], QUARTER[s]
        return jnp.concatenate([held[(1 + q) * unit : (2 + q) * unit], held[(3 + q) * unit : (4 + q) * unit]])

    f = all_ways(forwarded)
    g = all_ways(lambda ax, s: e[ax, s][QUARTER[s] * unit : (QUARTER[s] + 1) * unit])
    finals = placed([(d[w], d_places(*w)) for w in WAYS], unit, finals, widths)
    finals = placed([(c[w], c_places(*w)) for w in WAYS], unit, finals, widths)
    finals = placed([(e[w], e_places(*w)) for w in WAYS] + [(f[w], f_places(*w)) for w in WAYS], unit, finals, widths)
    finals = placed([(g[w], g_places(*w)) for w in WAYS], unit, finals, widths)
    return (*finals, *columns, gains)


def solution(mesh):
    return jax.shard_map(
        per_device,
        mesh=mesh,
        in_specs=(
            P("fsdp", "model"),
            P("fsdp", None),
            P(None, "model"),
            P("fsdp", "model"),
            P("fsdp", None),
            P(None, "model"),
            P("fsdp", "model"),
            P("fsdp", None),
            P(None, "model"),
            P(("fsdp", "model")),
            P(("fsdp", "model")),
        ),
        out_specs=(
            P(None, "model"),
            P(None, "model"),
            P(None, "model"),
            P("model"),
            P("model"),
            P("model"),
            P(),
        ),
        check_vma=False,
    )
```

```python
import jax
import jax.numpy as jnp
from jax import lax
from jax.experimental import pallas as pl
from jax.experimental.pallas import tpu as pltpu
from jax.sharding import PartitionSpec as P


mix_rate = 0.5
SIDE = 4
LANES = 128


def x_ring(step):
    return [(z * SIDE + x, z * SIDE + (x + step) % SIDE) for z in range(SIDE) for x in range(SIDE)]


def z_ring(step):
    return [(z * SIDE + x, (z + step) % SIDE * SIDE + x) for z in range(SIDE) for x in range(SIDE)]


RING = {"x": x_ring, "z": z_ring}


def wrapped(offset):
    return (offset + 1) % SIDE - 1


WAYS = [("x", 1), ("x", -1), ("z", 1), ("z", -1)]
LEAD = {"x": 0, "z": 1}
OTHER = {"x": "z", "z": "x"}
QUARTER = {1: 0, -1: 1}


def sent(array, axis, step):
    return lax.ppermute(array, "fsdp", RING[axis](step))


def all_ways(message):
    return {(ax, s): sent(message(ax, s), ax, s) for ax, s in WAYS}


def shifted(place, axis, step):
    ox, oz, h, k = place
    return (wrapped(ox - step), oz, h, k) if axis == "x" else (ox, wrapped(oz - step), h, k)


def pair(half, axis=None, step=0):
    places = [(0, 0, half, 0), (0, 0, half, 1)]
    return [shifted(p, axis, step) for p in places] if axis else places


def a_places(ax, s):
    return pair(LEAD[ax], ax, s)


def b_places(ax, s):
    return pair(1 - LEAD[ax], ax, s)


def c_message_places(ax, s):
    o = OTHER[ax]
    return [a_places(ax, s)[QUARTER[s]], *a_places(o, 1), *a_places(o, -1)]


def c_places(ax, s):
    return [shifted(p, ax, s) for p in c_message_places(ax, s)]


def d_places(ax, s):
    return [shifted(b_places(ax, s)[QUARTER[s]], ax, s)]


def e_message_places(ax):
    o = OTHER[ax]
    return [c_places(o, 1)[0], c_places(o, -1)[0]]


def e_places(ax, s):
    return [shifted(p, ax, s) for p in e_message_places(ax)]


def f_places(ax, s):
    held, q = c_places(ax, s), QUARTER[s]
    return [shifted(held[1 + q], ax, s), shifted(held[3 + q], ax, s)]


def g_places(ax, s):
    return [shifted(e_places(ax, s)[QUARTER[s]], ax, s)]


HBM = pl.BlockSpec(memory_space=pl.ANY)
VMEM = pl.BlockSpec(memory_space=pltpu.VMEM)


def in_vmem(array):
    return pltpu.with_memory_space_constraint(array, pltpu.VMEM)


def row_of(place, unit):
    me = lax.axis_index("fsdp")
    z, x = me // SIDE, me % SIDE
    ox, oz, h, k = place
    source = (z + oz + SIDE) % SIDE * SIDE + (x + ox + SIDE) % SIDE
    return pl.multiple_of((source * 4 + h * 2 + k) * unit, unit)


def runs(places):
    out, at = [], 0
    while at < len(places):
        ox, oz, h, k = places[at]
        size = 2 if k == 0 and at + 1 < len(places) and places[at + 1] == (ox, oz, h, 1) else 1
        out.append((at, size, places[at]))
        at += size
    return out


def column_copies(ref, first, rows, results, row, widths, sems):
    at = 0
    for n, width in enumerate(widths):
        pltpu.make_async_copy(
            ref.at[pl.ds(first, rows), pl.ds(at, width)], results[n].at[pl.ds(row, rows), :], sems.at[n]
        ).start()
        at += width


def wait_for(rows, results, sems):
    for n, result in enumerate(results):
        part = result.at[pl.ds(0, rows), :]
        pltpu.make_async_copy(part, part, sems.at[n]).wait()


def merged_into(raw, first, rows, mixed_ref, inverse_ref, targets, wide):
    low = raw[pl.ds(first, rows), pl.ds(wide, LANES)]
    tile = 2 * LANES
    for t in range(0, wide, tile):
        update = jnp.dot(low, mixed_ref[:, t : t + tile], preferred_element_type=jnp.float32)
        value = (raw[pl.ds(first, rows), t : t + tile].astype(jnp.float32) + update) * inverse_ref[:, t : t + tile]
        value = value.astype(jnp.bfloat16)
        for ref, at, skip, size in targets:
            ref[pl.ds(at, size), t : t + tile] = value[skip : skip + size]


def first_hop(a, unit, mixed, inverse, widths):
    wide, total = sum(widths), 4 * SIDE * SIDE * unit
    order = {way: n for n, way in enumerate(WAYS)}

    def body(*refs):
        mixed_ref, inverse_ref, raws = refs[0], refs[1], refs[2:6]
        messages, results, sems = refs[6:10], refs[10 : 10 + len(widths)], refs[-1]
        for ax, s in WAYS:
            o, q = OTHER[ax], QUARTER[s]
            at = (1 + 2 * q) * unit
            targets = [
                (messages[order[ax, s]], 0, q * unit, unit),
                (messages[order[o, 1]], at, 0, 2 * unit),
                (messages[order[o, -1]], at, 0, 2 * unit),
            ]
            merged_into(raws[order[ax, s]], 0, 2 * unit, mixed_ref, inverse_ref, targets, wide)
            column_copies(
                messages[order[o, 1]], at, 2 * unit, results, row_of(a_places(ax, s)[0], unit), widths, sems
            )
        wait_for(8 * unit, results, sems)

    out = pl.pallas_call(
        body,
        out_shape=[jax.ShapeDtypeStruct((5 * unit, wide), jnp.bfloat16)] * 4
        + [jax.ShapeDtypeStruct((total, width), jnp.bfloat16) for width in widths],
        in_specs=[VMEM] * 6,
        out_specs=[VMEM] * 4 + [HBM] * len(widths),
        scratch_shapes=[pltpu.SemaphoreType.DMA((len(widths),))],
        compiler_params=pltpu.CompilerParams(vmem_limit_bytes=8 * 2**20),
        name="first_hop",
    )(mixed, inverse, *[in_vmem(a[way]) for way in WAYS])
    return {way: out[n] for n, way in enumerate(WAYS)}, out[4:]


def second_hop(b, own, unit, mixed, inverse, finals, widths):
    wide = sum(widths)

    def body(*refs):
        mixed_ref, inverse_ref, raws, own_refs = refs[0], refs[1], refs[2:6], refs[6:8]
        messages = refs[8 + len(widths) : 12 + len(widths)]
        results, stage, sems = refs[12 + len(widths) : -2], refs[-2], refs[-1]
        for n, (ax, s) in enumerate(WAYS):
            q = QUARTER[s]
            at = 2 * n * unit
            targets = [(messages[n], 0, q * unit, unit), (stage, at, 0, 2 * unit)]
            merged_into(raws[n], 0, 2 * unit, mixed_ref, inverse_ref, targets, wide)
            column_copies(stage, at, 2 * unit, results, row_of(b_places(ax, s)[0], unit), widths, sems)
        for h in (0, 1):
            at = (8 + 2 * h) * unit
            merged_into(own_refs[h], 0, 2 * unit, mixed_ref, inverse_ref, [(stage, at, 0, 2 * unit)], wide)
            column_copies(stage, at, 2 * unit, results, row_of((0, 0, h, 0), unit), widths, sems)
        wait_for(12 * unit, results, sems)

    out = pl.pallas_call(
        body,
        out_shape=[jax.ShapeDtypeStruct((unit, wide), jnp.bfloat16)] * 4
        + [jax.ShapeDtypeStruct(f.shape, f.dtype) for f in finals],
        in_specs=[VMEM] * 8 + [HBM] * len(widths),
        out_specs=[VMEM] * 4 + [HBM] * len(widths),
        scratch_shapes=[pltpu.VMEM((12 * unit, wide), jnp.bfloat16), pltpu.SemaphoreType.DMA((len(widths),))],
        input_output_aliases={8 + n: 4 + n for n in range(len(widths))},
        compiler_params=pltpu.CompilerParams(vmem_limit_bytes=8 * 2**20),
        name="second_hop",
    )(mixed, inverse, *[in_vmem(b[way]) for way in WAYS], *[in_vmem(half) for half in own], *finals)
    return {way: out[n] for n, way in enumerate(WAYS)}, out[4:]


def placed(groups, unit, finals, widths):
    arrays = [array for array, _ in groups]
    count = len(arrays)

    def body(*refs):
        results, sems = refs[-1 - len(widths) : -1], refs[-1]
        rows = 0
        for ref, (_, places) in zip(refs[:count], groups):
            for at, size, place in runs(places):
                column_copies(ref, at * unit, size * unit, results, row_of(place, unit), widths, sems)
            rows += len(places) * unit
        wait_for(rows, results, sems)

    return pl.pallas_call(
        body,
        out_shape=[jax.ShapeDtypeStruct(f.shape, f.dtype) for f in finals],
        in_specs=[VMEM] * count + [HBM] * len(widths),
        out_specs=[HBM] * len(widths),
        scratch_shapes=[pltpu.SemaphoreType.DMA((len(widths),))],
        input_output_aliases={count + n: n for n in range(len(widths))},
        compiler_params=pltpu.CompilerParams(vmem_limit_bytes=8 * 2**20),
    )(*[in_vmem(array) for array in arrays], *finals)


def doubled_max(values):
    for bit in (SIDE, 3 * SIDE, 1, 3):
        other = lax.ppermute(values, "fsdp", [(i, i ^ bit) for i in range(SIDE * SIDE)])
        values = jnp.maximum(values, other)
    return values


def packed(weights, lows, highs, norms, widths):
    rows, wide = weights[0].shape[0], sum(widths)
    half, rank, count = rows // 2, lows[0].shape[1], len(weights)
    tile, deep = 2 * LANES, LANES // 2
    cell = norms[0].shape

    def body(*refs):
        sources, turned, factors = refs[:count], refs[count : 2 * count], refs[2 * count : 3 * count]
        outs, largest, spreads = refs[3 * count + 2 : 3 * count + 4], refs[3 * count + 4], refs[3 * count + 5 : 3 * count + 7]
        gain, stage, held, sems = refs[-4:]
        norm_copies = [
            pltpu.make_async_copy(refs[3 * count + n], held.at[n], sems.at[4 * count + n]) for n in (0, 1)
        ]
        for copy in norm_copies:
            copy.start()
        low_copies = [pltpu.make_async_copy(turned[n], stage.at[n], sems.at[n]) for n in range(count)]
        for copy in low_copies:
            copy.start()
        copies, at = [], 0
        for n, width in enumerate(widths):
            for h in (0, 1):
                copies.append(
                    pltpu.make_async_copy(
                        sources[n].at[pl.ds(h * half, half), :],
                        outs[h].at[:, pl.ds(at, width)],
                        sems.at[count + 2 * n + h],
                    )
                )
                copies[-1].start()
            at += width
        for part in spreads:
            part[...] = jnp.zeros(part.shape, part.dtype)
        at = 0
        for n, width in enumerate(widths):
            copies.append(
                pltpu.make_async_copy(
                    factors[n],
                    spreads[n * rank // deep].at[pl.ds(n * rank % deep, rank), pl.ds(at, width)],
                    sems.at[3 * count + n],
                )
            )
            copies[-1].start()
            at += width
        for copy in low_copies:
            copy.wait()
        low = jnp.concatenate(
            [stage[n].astype(jnp.float32) for n in range(count)]
            + [jnp.zeros((LANES - count * rank, rows), jnp.float32)]
        )
        straight = low.T.astype(stage.dtype)
        for h in (0, 1):
            outs[h][:, wide:] = straight[h * half : (h + 1) * half]
        for copy in copies:
            copy.wait()
        for t in range(0, wide, tile):
            best = None
            factor = jnp.concatenate([part[:, t : t + tile] for part in spreads])
            for h in (0, 1):
                update = jnp.dot(outs[h][:, wide:], factor, preferred_element_type=jnp.float32)
                value = jnp.abs(outs[h][:, t : t + tile].astype(jnp.float32) + mix_rate * update)
                value = jnp.max(value, axis=0, keepdims=True)
                best = value if best is None else jnp.maximum(best, value)
            largest[:, t : t + tile] = best
        for copy in norm_copies:
            copy.wait()
        gain[...] = (held[0] + held[1]).astype(jnp.bfloat16).astype(jnp.float32)

    hbm = pltpu.MemorySpace.HBM
    return pl.pallas_call(
        body,
        out_shape=[jax.ShapeDtypeStruct((half, wide + LANES), jnp.bfloat16)] * 2
        + [jax.ShapeDtypeStruct((1, wide), jnp.float32)]
        + [jax.ShapeDtypeStruct((deep, wide), jnp.bfloat16)] * 2
        + [jax.ShapeDtypeStruct(cell, jnp.float32)],
        in_specs=[pl.BlockSpec(memory_space=hbm)] * (3 * count + 2),
        out_specs=[VMEM] * 6,
        scratch_shapes=[
            pltpu.VMEM((count, rank, rows), jnp.bfloat16),
            pltpu.VMEM((2, *cell), jnp.float32),
            pltpu.SemaphoreType.DMA((4 * count + 2,)),
        ],
        compiler_params=pltpu.CompilerParams(vmem_limit_bytes=4 * 2**20),
        name="packed",
    )(*[pltpu.with_memory_space_constraint(a, hbm) for a in (*weights, *[low.T for low in lows], *highs, *norms)])


def per_device(
    weight_query,
    low_query,
    high_query,
    weight_key,
    low_key,
    high_key,
    weight_value,
    low_value,
    high_value,
    norm_train,
    norm_step,
):
    me = lax.axis_index("fsdp")
    lane = lax.axis_index("model")
    groups, lanes = lax.axis_size("fsdp"), lax.axis_size("model")
    weights = (weight_query, weight_key, weight_value)
    lows = (low_query, low_key, low_value)
    highs = (high_query, high_key, high_value)
    widths = [w.shape[1] for w in weights]
    wide = sum(widths)
    rows = weight_query.shape[0]
    unit = rows // 4
    *halves, largest, spread_0, spread_1, norm = packed(
        weights, lows, highs, [n.reshape(1, -1) for n in (norm_train, norm_step)], widths
    )
    size = norm.shape[1]
    slots = lax.dynamic_update_slice(
        jnp.full((groups * lanes * size,), -jnp.inf), norm.reshape(-1), ((me * lanes + lane) * size,)
    )
    a = all_ways(lambda ax, s: halves[LEAD[ax]])
    b = all_ways(lambda ax, s: halves[1 - LEAD[ax]])

    shared = doubled_max(jnp.concatenate([largest.reshape(-1), slots]))
    columns, at = [], 0
    for width in widths:
        columns.append(shared[at : at + width])
        at += width
    inverse = (1.0 / shared[:wide]).reshape(1, wide)
    scaled_0 = mix_rate * spread_0
    scaled_1 = mix_rate * spread_1
    mixed = jnp.concatenate([scaled_0, scaled_1])

    messages, finals = first_hop(a, unit, mixed, inverse, widths)
    c = all_ways(lambda ax, s: messages[ax, s])
    messages, finals = second_hop(b, halves, unit, mixed, inverse, finals, widths)
    d = all_ways(lambda ax, s: messages[ax, s])

    gains = shared[wide:]
    for n in range(3):
        other = lax.ppermute(gains, "model", [(i, i ^ (1, 2, 6)[n]) for i in range(lanes)])
        gains = jnp.maximum(gains, other)
        if n == 2:
            gains = gains.astype(jnp.bfloat16)

    along = {ax: jnp.concatenate([c[OTHER[ax], 1][:unit], c[OTHER[ax], -1][:unit]]) for ax in "xz"}
    e = all_ways(lambda ax, s: along[ax])

    def forwarded(ax, s):
        held, q = c[ax, s], QUARTER[s]
        return jnp.concatenate([held[(1 + q) * unit : (2 + q) * unit], held[(3 + q) * unit : (4 + q) * unit]])

    f = all_ways(forwarded)
    g = all_ways(lambda ax, s: e[ax, s][QUARTER[s] * unit : (QUARTER[s] + 1) * unit])
    finals = placed([(d[w], d_places(*w)) for w in WAYS], unit, finals, widths)
    finals = placed([(c[w], c_places(*w)) for w in WAYS], unit, finals, widths)
    finals = placed([(e[w], e_places(*w)) for w in WAYS] + [(f[w], f_places(*w)) for w in WAYS], unit, finals, widths)
    finals = placed([(g[w], g_places(*w)) for w in WAYS], unit, finals, widths)
    return (*finals, *columns, gains)


def solution(mesh):
    return jax.shard_map(
        per_device,
        mesh=mesh,
        in_specs=(
            P("fsdp", "model"),
            P("fsdp", None),
            P(None, "model"),
            P("fsdp", "model"),
            P("fsdp", None),
            P(None, "model"),
            P("fsdp", "model"),
            P("fsdp", None),
            P(None, "model"),
            P(("fsdp", "model")),
            P(("fsdp", "model")),
        ),
        out_specs=(
            P(None, "model"),
            P(None, "model"),
            P(None, "model"),
            P("model"),
            P("model"),
            P("model"),
            P(),
        ),
        check_vma=False,
    )
```
